32 devices in a mesh: data: 4 (over y, z), seq: 8 (over x, core).
Axes of the slice: x: 4, y: 2, z: 2, core: 2. Of those that a mesh axis runs over, the one named last changes fastest.
The devices are a block of a 4x4x8 slice.
Arguments:
- act_in: bfloat16 [16, 2048, 1280], P('data', 'seq'), parts along dimension 0
- ln1_scale: float32 [1280], replicated
- ln1_bias: float32 [1280], replicated
- w_in: bfloat16 [1280, 5120], replicated
- b_in: float32 [5120], replicated
- ln2_scale: float32 [2560], replicated
- ln2_bias: float32 [2560], replicated
- w_spatial: bfloat16 [2048, 2048], replicated
- b_spatial: float32 [2048], replicated
- causal_mask: int32 [2048, 2048], replicated
- w_out: bfloat16 [2560, 1280], replicated
- b_out: float32 [1280], replicated
Outputs:
- output: bfloat16 [16, 2048, 1280], P('data', 'seq'), parts along dimension 0
There are 4 independent parts. The reference program is written for one: setup_inputs(seed, part) draws one part's arguments, and reference() takes and returns one part's arrays. A program takes and returns all parts, laid end to end along the dimension named above; an argument that names none is the same for every part.
All inputs are finite; a program needn't handle non-finite values.
Results may differ from the reference program's by a relative error of at most 0.011577.
Values are sent between devices in bfloat16 or wider.
A program may use at most 768 MiB of HBM per device.

```python
import jax
import jax.numpy as jnp
from jax import lax

BATCH_ROWS = 4
SEQ_LEN = 2048
MODEL_DIM = 1280
FFN_DIM = 5120
GATE_DIM = FFN_DIM // 2
LN_EPS = 1e-6


def layer_norm(features, ln_gain, ln_shift):
    mean_val = jnp.mean(features, axis=-1, keepdims=True)
    centered = features - mean_val
    var_val = jnp.mean(centered * centered, axis=-1, keepdims=True)
    return centered * lax.rsqrt(var_val + LN_EPS) * ln_gain + ln_shift


def draw_mask(mask_key):
    cut_points = jax.random.randint(mask_key, (2,), 1, SEQ_LEN)
    positions = jnp.arange(SEQ_LEN)
    doc_id = jnp.sum(positions[:, None] >= cut_points[None, :], axis=1)
    keep_mask = (positions[None, :] <= positions[:, None]) & (doc_id[None, :] == doc_id[:, None])
    return keep_mask.astype(jnp.int32)


def setup_inputs(seed: int = 0, part: int = 0) -> dict:
    key_list = jax.random.split(jax.random.key(seed), 12)
    x_key = jax.random.fold_in(key_list[0], part)
    causal_mask = draw_mask(key_list[7])
    row_count = jnp.sum(causal_mask, axis=1).astype(jnp.float32)
    act_in = jax.random.normal(x_key, (BATCH_ROWS, SEQ_LEN, MODEL_DIM), jnp.float32)
    ln1_scale = 1.0 + 0.5 * jax.random.normal(key_list[1], (MODEL_DIM,), jnp.float32)
    ln1_bias = 0.5 * jax.random.normal(key_list[2], (MODEL_DIM,), jnp.float32)
    w_in = jax.random.normal(key_list[3], (MODEL_DIM, FFN_DIM), jnp.float32) * MODEL_DIM ** -0.5
    b_in = 0.5 * jax.random.normal(key_list[4], (FFN_DIM,), jnp.float32)
    ln2_scale = 1.0 + 0.5 * jax.random.normal(key_list[5], (GATE_DIM,), jnp.float32)
    ln2_bias = 0.5 * jax.random.normal(key_list[6], (GATE_DIM,), jnp.float32)
    w_spatial = jax.random.normal(key_list[8], (SEQ_LEN, SEQ_LEN), jnp.float32) * lax.rsqrt(row_count)[:, None]
    b_spatial = 1.0 + 0.8 * jax.random.normal(key_list[9], (SEQ_LEN,), jnp.float32)
    w_out = jax.random.normal(key_list[10], (GATE_DIM, MODEL_DIM), jnp.float32) * (2.0 * GATE_DIM ** -0.5)
    b_out = 0.3 * jax.random.normal(key_list[11], (MODEL_DIM,), jnp.float32)
    return dict(
        act_in=act_in.astype(jnp.bfloat16),
        ln1_scale=ln1_scale,
        ln1_bias=ln1_bias,
        w_in=w_in.astype(jnp.bfloat16),
        b_in=b_in,
        ln2_scale=ln2_scale,
        ln2_bias=ln2_bias,
        w_spatial=w_spatial.astype(jnp.bfloat16),
        b_spatial=b_spatial,
        causal_mask=causal_mask,
        w_out=w_out.astype(jnp.bfloat16),
        b_out=b_out,
    )


def reference(act_in, ln1_scale, ln1_bias, w_in, b_in, ln2_scale, ln2_bias, w_spatial, b_spatial, causal_mask, w_out, b_out):
    w_masked = jnp.where(causal_mask > 0, w_spatial, jnp.zeros_like(w_spatial))

    def one_sequence(seq_act):
        normed = layer_norm(seq_act.astype(jnp.float32), ln1_scale, ln1_bias).astype(jnp.bfloat16)
        hidden = jax.nn.gelu(jnp.dot(normed, w_in, preferred_element_type=jnp.float32) + b_in, approximate=True).astype(jnp.bfloat16)
        gate_half = hidden[:, :GATE_DIM]
        value_norm = layer_norm(hidden[:, GATE_DIM:].astype(jnp.float32), ln2_scale, ln2_bias).astype(jnp.bfloat16)
        spatial = (jnp.dot(w_masked, value_norm, preferred_element_type=jnp.float32) + b_spatial[:, None]).astype(jnp.bfloat16)
        gated_act = (gate_half.astype(jnp.float32) * spatial.astype(jnp.float32)).astype(jnp.bfloat16)
        projected = jnp.dot(gated_act, w_out, preferred_element_type=jnp.float32) + b_out
        return (seq_act.astype(jnp.float32) + projected).astype(jnp.bfloat16)

    return lax.map(one_sequence, act_in)
```

```python
import functools

import jax
import jax.numpy as jnp
from jax import lax
from jax.experimental import pallas as pl
from jax.experimental.pallas import tpu as pltpu
from jax.sharding import PartitionSpec as P

LN_EPS = 1e-6
MESH = pl.DeviceIdType.MESH
GELU_A = 0.7978845608028654
GELU_B = 0.7978845608028654 * 0.044715
CORES = 2
NT = 512
OT = 256


def gelu(a):
    return (0.5 * a) * (1.0 + jnp.tanh(a * (GELU_A + GELU_B * (a * a))))


def block_kernel(chips, x_hbm, ln1s, ln1b, w_in_hbm, b_in, ln2s, ln2b, w_sp_hbm, b_sp, mask_hbm, w_out_hbm, b_out,
                 out_hbm,
                 w_in, w_out, xg, u, v, g, vn, wm, mk, q, o, bs,
                 w_in_sem, w_out_sem, wm_sem, mk_sem, own_sem, x_send, x_recv, v_send, v_recv, o_send, o_recv, o_loc):
    rows, model = x_hbm.shape[1:]
    gate = w_out.shape[0]
    n_in = gate // NT
    n_out = model // OT
    span = CORES * rows
    data = lax.axis_index("data")
    me = lax.axis_index("seq")
    chip = me // CORES
    core = me % CORES

    def device(c):
        return (data, c * CORES + core)

    partner = (data, chip * CORES + (1 - core))

    barrier = pltpu.get_barrier_semaphore()
    for d in range(1, chips):
        pl.semaphore_signal(barrier, inc=1, device_id=device((chip + d) % chips), device_id_type=MESH)
    pl.semaphore_signal(barrier, inc=1, device_id=partner, device_id_type=MESH)

    own_copy = pltpu.make_async_copy(x_hbm.at[chip], xg.at[chip], own_sem)
    own_copy.start()

    def w_in_copy(n):
        cols = pl.ds(pl.multiple_of(n * NT, NT), NT)
        return pltpu.make_async_copy(w_in_hbm.at[:, cols], w_in.at[:, cols], w_in_sem.at[n])

    for n in range(n_in):
        w_in_copy(n_in + n).start()

    pl.semaphore_wait(barrier, chips)

    def x_copy(d):
        to = (chip + d) % chips
        return pltpu.make_async_remote_copy(
            src_ref=x_hbm.at[to], dst_ref=xg.at[chip], send_sem=x_send.at[d], recv_sem=x_recv.at[d],
            device_id=device(to), device_id_type=MESH)

    for d in (2, 1, 3):
        x_copy(d).start()

    for n in range(n_in):
        w_in_copy(n).start()
    wm_copies, mk_copies = [], []
    t = 0
    for i in range(chips):
        r = pl.ds(pl.multiple_of((CORES * i + core) * rows, rows), rows)
        cp = pltpu.make_async_copy(w_sp_hbm.at[r, pl.ds(0, span * (i + 1))], wm.at[i, :, pl.ds(0, span * (i + 1))],
                                   wm_sem.at[i])
        cp.start()
        wm_copies.append(cp)
        for j in range(i + 1):
            cp = pltpu.make_async_copy(mask_hbm.at[r, pl.ds(span * j, span)], mk.at[t], mk_sem.at[t])
            cp.start()
            mk_copies.append(cp)
            t += 1
    w_out_copy = pltpu.make_async_copy(w_out_hbm, w_out, w_out_sem)
    w_out_copy.start()

    def hidden(k, j):
        own_rows = pl.multiple_of((CORES * j + core) * rows, rows)

        @pl.loop(0, rows // 32)
        def _(r):
            rr = pl.ds(pl.multiple_of(r * 32, 32), 32)
            xf = xg[j, rr, :].astype(jnp.float32)
            c = xf - jnp.mean(xf, axis=-1, keepdims=True)
            var = jnp.mean(c * c, axis=-1, keepdims=True)
            u[rr, :] = (c * lax.rsqrt(var + LN_EPS) * ln1s[...] + ln1b[...]).astype(jnp.bfloat16)

        @pl.loop(0, n_in)
        def _(n):
            @pl.when(k == 0)
            def _():
                w_in_copy(n_in + n).wait()

            cols = pl.ds(pl.multiple_of(n * NT, NT), NT)
            wcols = pl.ds(pl.multiple_of(gate + n * NT, NT), NT)
            a = jnp.dot(u[...], w_in[:, wcols], preferred_element_type=jnp.float32) + b_in[:, wcols]
            v[:, cols] = gelu(a).astype(jnp.bfloat16)

        @pl.loop(0, rows // 16)
        def _(r):
            rr = pl.ds(pl.multiple_of(r * 16, 16), 16)
            vf = v[rr, :].astype(jnp.float32)
            c = vf - jnp.mean(vf, axis=-1, keepdims=True)
            var = jnp.mean(c * c, axis=-1, keepdims=True)
            y = (c * lax.rsqrt(var + LN_EPS) * ln2s[...] + ln2b[...]).astype(jnp.bfloat16)
            vn[pl.ds(pl.multiple_of(own_rows + r * 16, 16), 16), :] = y

        @pl.loop(0, n_in)
        def _(n):
            @pl.when(k == 0)
            def _():
                w_in_copy(n).wait()

            cols = pl.ds(pl.multiple_of(n * NT, NT), NT)
            a = jnp.dot(u[...], w_in[:, cols], preferred_element_type=jnp.float32) + b_in[:, cols]
            g[j, :, cols] = gelu(a).astype(jnp.bfloat16)

            @pl.when(n == 0)
            def _():
                vn_copy(k, j).start()

    def vn_copy(k, j):
        r = pl.ds(pl.multiple_of((CORES * j + core) * rows, rows), rows)
        return pltpu.make_async_remote_copy(
            src_ref=vn.at[r], dst_ref=vn.at[r], send_sem=v_send.at[k], recv_sem=v_recv.at[k],
            device_id=partner, device_id_type=MESH)

    def mask_weights():
        for cp in wm_copies + mk_copies:
            cp.wait()
        t = 0
        for i in range(chips):
            for j in range(i + 1):
                cols = pl.ds(span * j, span)

                @pl.loop(0, rows // 32)
                def _(r, i=i, t=t, cols=cols):
                    rr = pl.ds(pl.multiple_of(r * 32, 32), 32)
                    w = wm[i, rr, cols].astype(jnp.float32)
                    wm[i, rr, cols] = jnp.where(mk[t, rr, :] > 0, w, 0.0).astype(jnp.bfloat16)

                t += 1
            row = b_sp[pl.ds(CORES * i + core, 1), :]
            bs[i, :, :] = jnp.transpose(jnp.broadcast_to(row, (128, rows)))

    def o_copy(i, n, recv):
        cols = pl.ds(pl.multiple_of(n * OT, OT), OT)
        return pltpu.make_async_remote_copy(
            src_ref=o.at[i, :, cols], dst_ref=out_hbm.at[chip, :, cols], send_sem=o_send.at[i, n],
            recv_sem=o_recv.at[recv, n], device_id=device(i), device_id_type=MESH)

    def o_local(n):
        cols = pl.ds(pl.multiple_of(n * OT, OT), OT)
        return pltpu.make_async_copy(o.at[chip, :, cols], out_hbm.at[chip, :, cols], o_loc.at[n])

    def mix(k, i):
        for s in range(chips):
            @pl.when(i == s)
            def _(s=s):
                depth = span * (s + 1)

                @pl.loop(0, n_in)
                def _(n):
                    cols = pl.ds(pl.multiple_of(n * NT, NT), NT)
                    acc = jnp.dot(wm[s, :, pl.ds(0, depth)], vn[pl.ds(0, depth), cols],
                                  preferred_element_type=jnp.float32)
                    sp = (acc + bs[s, :, 0:1]).astype(jnp.bfloat16).astype(jnp.float32)
                    q[:, cols] = (g[s, :, cols].astype(jnp.float32) * sp).astype(jnp.bfloat16)

        @pl.when(k == 1)
        def _():
            w_out_copy.wait()

        @pl.loop(0, n_out)
        def _(n):
            cols = pl.ds(pl.multiple_of(n * OT, OT), OT)
            y = jnp.dot(q[...], w_out[:, cols], preferred_element_type=jnp.float32) + b_out[:, cols]
            o[i, :, cols] = (xg[i, :, cols].astype(jnp.float32) + y).astype(jnp.bfloat16)

            @pl.when(k < chips)
            def _():
                o_copy(i, n, chip).start()

            @pl.when(k == chips)
            def _():
                o_local(n).start()

    def other(k):
        return (k - 1) + jnp.where(k - 1 >= chip, 1, 0)

    own_copy.wait()

    @pl.loop(0, chips + 1)
    def _(k):
        @pl.when(k == 0)
        def _():
            hidden(k, chip)
            mask_weights()

        @pl.when((k >= 1) & (k < chips))
        def _():
            j = other(k)
            x_copy((chip - j + chips) % chips).wait_recv()
            hidden(k, j)

            @pl.when(k == 1)
            def _():
                vn_copy(0, chip).wait_recv()

            vn_copy(k, j).wait_recv()

        @pl.when(k >= 1)
        def _():
            mix(k, jnp.where(k < chips, other(k), chip))

    for d in range(1, chips):
        x_copy(d).wait_send()
        src = (chip - d + chips) % chips
        for n in range(n_out):
            o_copy(src, n, chip).wait_send()
            o_copy(src, n, src).wait_recv()
    for n in range(n_out):
        o_local(n).wait()
    vn_copy(0, chip).wait_send()
    for k in range(1, chips):
        vn_copy(k, other(k)).wait_send()


def solution(mesh):
    row_spec = P('data', 'seq', None)
    chips = mesh.shape['seq'] // CORES

    def local_block(act_in, ln1_scale, ln1_bias, w_in, b_in, ln2_scale, ln2_bias, w_spatial, b_spatial, causal_mask, w_out, b_out):
        batch, rows, model = act_in.shape
        ffn = w_in.shape[1]
        gate = w_out.shape[0]
        seq = w_spatial.shape[0]
        span = CORES * rows
        assert batch == chips and span * chips == seq
        n_in, n_out = gate // NT, model // OT
        tiles = chips * (chips + 1) // 2
        hbm = pl.BlockSpec(memory_space=pl.ANY)
        vmem = pl.BlockSpec(memory_space=pltpu.VMEM)
        bf, f32 = jnp.bfloat16, jnp.float32
        dma = pltpu.SemaphoreType.DMA
        return pl.pallas_call(
            functools.partial(block_kernel, chips),
            out_shape=jax.ShapeDtypeStruct(act_in.shape, bf),
            in_specs=[hbm, vmem, vmem, hbm, vmem, vmem, vmem, hbm, vmem, hbm, hbm, vmem],
            out_specs=hbm,
            scratch_shapes=[
                pltpu.VMEM((model, ffn), bf),
                pltpu.VMEM((gate, model), bf),
                pltpu.VMEM((chips, rows, model), bf),
                pltpu.VMEM((rows, model), bf),
                pltpu.VMEM((rows, gate), bf),
                pltpu.VMEM((chips, rows, gate), bf),
                pltpu.VMEM((seq, gate), bf),
                pltpu.VMEM((chips, rows, seq), bf),
                pltpu.VMEM((tiles, rows, span), jnp.int32),
                pltpu.VMEM((rows, gate), bf),
                pltpu.VMEM((chips, rows, model), bf),
                pltpu.VMEM((chips, rows, 128), f32),
                dma((2 * n_in,)), dma, dma((chips,)), dma((tiles,)), dma,
                dma((chips,)), dma((chips,)), dma((chips,)), dma((chips,)),
                dma((chips, n_out)), dma((chips, n_out)), dma((n_out,)),
            ],
            compiler_params=pltpu.CompilerParams(collective_id=0, has_side_effects=True,
                                                 vmem_limit_bytes=66 * 1000 * 1000),
            name="gmlp_block",
        )(act_in, ln1_scale.reshape(1, -1), ln1_bias.reshape(1, -1), w_in, b_in.reshape(1, -1),
          ln2_scale.reshape(1, -1), ln2_bias.reshape(1, -1), w_spatial, b_spatial.reshape(-1, rows), causal_mask,
          w_out, b_out.reshape(1, -1))

    return jax.shard_map(local_block, mesh=mesh, in_specs=(row_spec,) + (P(),) * 11, out_specs=row_spec, check_vma=False)
```

```python
import functools

import jax
import jax.numpy as jnp
from jax import lax
from jax.experimental import pallas as pl
from jax.experimental.pallas import tpu as pltpu
from jax.sharding import PartitionSpec as P

LN_EPS = 1e-6
MESH = pl.DeviceIdType.MESH
GELU_A = 0.7978845608028654
GELU_B = 0.7978845608028654 * 0.044715
CORES = 2
NT = 512
OT = 256
PLANS = [
    [0, 1, 5, 3, 2, 6, 7, 4],
    [1, 0, 4, 2, 6, 3, 7, 5],
    [2, 1, 3, 0, 4, 5, 7, 6],
    [3, 0, 4, 2, 1, 5, 6, 7],
]


def gelu(a):
    return (0.5 * a) * (1.0 + jnp.tanh(a * (GELU_A + GELU_B * (a * a))))


def norm_rows(src, dst, at, groups, width, scale, shift):
    tiles = [slice(t * 128, (t + 1) * 128) for t in range(width // 128)]
    rows = [pl.ds(pl.multiple_of(at[0] + 32 * r, 32), 32) for r in range(groups)]
    to = [pl.ds(pl.multiple_of(at[1] + 32 * r, 32), 32) for r in range(groups)]

    def total(parts):
        acc = parts[0]
        for p in parts[1:]:
            acc = acc + p
        return jnp.sum(acc, axis=-1, keepdims=True) * (1.0 / width)

    def load(r, t):
        return src[r, t].astype(jnp.float32)

    mean = [total([load(r, t) for t in tiles]) for r in rows]
    inv = []
    for r, m in zip(rows, mean):
        inv.append(lax.rsqrt(total([(load(r, t) - m) * (load(r, t) - m) for t in tiles]) + LN_EPS))
    for r, m, s, d in zip(rows, mean, inv, to):
        for t in tiles:
            dst[d, t] = ((load(r, t) - m) * s * scale[:, t] + shift[:, t]).astype(jnp.bfloat16)


def by_chip(chip, values):
    out = values[-1]
    for c in range(len(values) - 1):
        out = jnp.where(chip == c, values[c], out)
    return out


def block_kernel(chips, x_hbm, ln1s_1d, ln1b_1d, w_in_hbm, b_in_1d, ln2s_1d, ln2b_1d, w_sp_hbm, b_sp_1d, mask_hbm,
                 w_out_hbm, b_out_1d, out_hbm,
                 w_in, w_out, xg, u, v, g, vn, wm, mk, q, o, bs, ln1s, ln1b, b_in, ln2s, ln2b, b_out,
                 w_in_sem, w_out_sem, wm_sem, mk_sem, own_sem, x_send, x_recv, v_send, v_recv, o_send, o_recv, o_loc):
    rows, model = x_hbm.shape[1:]
    gate = w_out.shape[0]
    n_in = gate // NT
    span = CORES * rows
    data = lax.axis_index("data")
    me = lax.axis_index("seq")
    chip = me // CORES
    core = me % CORES

    def device(c):
        return (data, c * CORES + core)

    partner = (data, chip * CORES + (1 - core))

    barrier = pltpu.get_barrier_semaphore()
    for d in range(1, chips):
        pl.semaphore_signal(barrier, inc=1, device_id=device((chip + d) % chips), device_id_type=MESH)
    pl.semaphore_signal(barrier, inc=1, device_id=partner, device_id_type=MESH)

    own_copy = pltpu.make_async_copy(x_hbm.at[chip], xg.at[chip], own_sem)
    own_copy.start()
    w_in_copies = []
    for n in range(2):
        cols = pl.ds(gate * (1 - n), gate)
        w_in_copies.append(pltpu.make_async_copy(w_in_hbm.at[:, cols], w_in.at[:, cols], w_in_sem.at[n]))
    w_in_copies[0].start()
    for src, dst in ((ln1s_1d, ln1s), (ln1b_1d, ln1b), (b_in_1d, b_in), (ln2s_1d, ln2s), (ln2b_1d, ln2b),
                     (b_out_1d, b_out)):
        dst[...] = src[...].reshape(1, -1)

    pl.semaphore_wait(barrier, chips)

    def x_copy(d):
        to = (chip + d) % chips
        return pltpu.make_async_remote_copy(
            src_ref=x_hbm.at[to], dst_ref=xg.at[chip], send_sem=x_send.at[d], recv_sem=x_recv.at[d],
            device_id=device(to), device_id_type=MESH)

    for d in (1, 3, 2):
        x_copy(d).start()

    w_in_copies[1].start()
    wm_copies, mk_copies = [], []
    t = 0
    for i in range(chips):
        r = pl.ds(pl.multiple_of((CORES * i + core) * rows, rows), rows)
        cp = pltpu.make_async_copy(w_sp_hbm.at[r, pl.ds(0, span * (i + 1))], wm.at[i, :, pl.ds(0, span * (i + 1))],
                                   wm_sem.at[i])
        cp.start()
        wm_copies.append(cp)
        for j in range(i + 1):
            cp = pltpu.make_async_copy(mask_hbm.at[r, pl.ds(span * j, span)], mk.at[t], mk_sem.at[t])
            cp.start()
            mk_copies.append(cp)
            t += 1
    w_out_copy = pltpu.make_async_copy(w_out_hbm, w_out, w_out_sem)
    w_out_copy.start()

    def vn_copy(j):
        r = pl.ds(pl.multiple_of((CORES * j + core) * rows, rows), rows)
        return pltpu.make_async_remote_copy(
            src_ref=vn.at[r], dst_ref=vn.at[r], send_sem=v_send.at[j], recv_sem=v_recv.at[j],
            device_id=partner, device_id_type=MESH)

    def hidden(k, j):
        @pl.when(k == 0)
        def _():
            own_copy.wait()
            w_in_copies[0].wait()

        @pl.when(k > 0)
        def _():
            x_copy((chip - j + chips) % chips).wait_recv()

        norm_rows(xg.at[j], u, (0, 0), rows // 32, model, ln1s, ln1b)

        def half(dst, base, n):
            cols = slice(n * NT, (n + 1) * NT)
            wcols = slice(base + n * NT, base + (n + 1) * NT)
            a = jnp.dot(u[...], w_in[:, wcols], preferred_element_type=jnp.float32) + b_in[:, wcols]
            dst[:, cols] = gelu(a).astype(jnp.bfloat16)

        for n in range(n_in):
            half(v, gate, n)

        own_rows = (CORES * j + core) * rows

        @pl.loop(0, 2)
        def _(r):
            norm_rows(v, vn, (r * 128, own_rows + r * 128), 4, gate, ln2s, ln2b)

        @pl.when(k == 0)
        def _():
            w_in_copies[1].wait()

        half(g.at[j], 0, 0)
        vn_copy(j).start()
        for n in range(1, n_in):
            half(g.at[j], 0, n)

    def mask_weights():
        for cp in wm_copies + mk_copies:
            cp.wait()
        t = 0
        for i in range(chips):
            for j in range(i + 1):
                cols = pl.ds(span * j, span)

                @pl.loop(0, rows // 32)
                def _(r, i=i, t=t, cols=cols):
                    rr = pl.ds(pl.multiple_of(r * 32, 32), 32)
                    w = wm[i, rr, cols].astype(jnp.float32)
                    wm[i, rr, cols] = jnp.where(mk[t, rr, :] > 0, w, 0.0).astype(jnp.bfloat16)

                t += 1
            row = b_sp_1d[pl.ds(pl.multiple_of((CORES * i + core) * rows, rows), rows)].reshape(1, rows)
            bs[i, :, :] = jnp.transpose(jnp.broadcast_to(row, (128, rows)))

    cuts = [(0, 768), (768, model)] if model > 768 else [(0, model)]

    def o_copy(i, n, recv):
        cols = pl.ds(cuts[n][0], cuts[n][1] - cuts[n][0])
        return pltpu.make_async_remote_copy(
            src_ref=o.at[i, :, cols], dst_ref=out_hbm.at[chip, :, cols], send_sem=o_send.at[i, n],
            recv_sem=o_recv.at[recv, n], device_id=device(i), device_id_type=MESH)

    def o_local(n):
        cols = pl.ds(cuts[n][0], cuts[n][1] - cuts[n][0])
        return pltpu.make_async_copy(o.at[chip, :, cols], out_hbm.at[chip, :, cols], o_loc.at[n])

    def mix(i):
        @pl.when(i != chip)
        def _():
            vn_copy(i).wait_recv()

        @pl.when(i == chip + 1)
        def _():
            vn_copy(chip).wait_recv()

        @pl.when((i == chip) & (i == chips - 1))
        def _():
            vn_copy(chip).wait_recv()

        for s in range(chips):
            @pl.when(i == s)
            def _(s=s):
                depth = span * (s + 1)
                for n in range(n_in):
                    cols = slice(n * NT, (n + 1) * NT)
                    acc = jnp.dot(wm[s, :, :depth], vn[:depth, cols], preferred_element_type=jnp.float32)
                    sp = (acc + bs[s, :, 0:1]).astype(jnp.bfloat16).astype(jnp.float32)
                    q[:, cols] = (g[s, :, cols].astype(jnp.float32) * sp).astype(jnp.bfloat16)

        for n, (lo, hi) in enumerate(cuts):
            for c in range(lo, hi, OT):
                cols = slice(c, c + OT)
                y = jnp.dot(q[...], w_out[:, cols], preferred_element_type=jnp.float32) + b_out[:, cols]
                o[i, :, cols] = (xg[i, :, cols].astype(jnp.float32) + y).astype(jnp.bfloat16)

            @pl.when(i != chip)
            def _(n=n):
                o_copy(i, n, chip).start()

            @pl.when(i == chip)
            def _(n=n):
                o_local(n).start()

    plans = by_chip(chip, [sum(op << (3 * k) for k, op in enumerate(p)) for p in PLANS])

    @pl.loop(0, 2 * chips)
    def _(k):
        op = lax.shift_right_logical(plans, 3 * k) % 8

        @pl.when(op < chips)
        def _():
            hidden(k, op)

        @pl.when(k == 0)
        def _():
            mask_weights()
            w_out_copy.wait()

        @pl.when(op >= chips)
        def _():
            mix(op - chips)

    for d in range(1, chips):
        x_copy(d).wait_send()
        src = (chip - d + chips) % chips
        for n in range(len(cuts)):
            o_copy(src, n, chip).wait_send()
            o_copy(src, n, src).wait_recv()
    for n in range(len(cuts)):
        o_local(n).wait()
    for j in range(chips):
        vn_copy(j).wait_send()


def solution(mesh):
    row_spec = P('data', 'seq', None)
    chips = mesh.shape['seq'] // CORES

    def local_block(act_in, ln1_scale, ln1_bias, w_in, b_in, ln2_scale, ln2_bias, w_spatial, b_spatial, causal_mask, w_out, b_out):
        batch, rows, model = act_in.shape
        ffn = w_in.shape[1]
        gate = w_out.shape[0]
        seq = w_spatial.shape[0]
        span = CORES * rows
        assert batch == chips and span * chips == seq
        n_out = 2 if model > 768 else 1
        tiles = chips * (chips + 1) // 2
        hbm = pl.BlockSpec(memory_space=pl.ANY)
        vmem = pl.BlockSpec(memory_space=pltpu.VMEM)
        bf, f32 = jnp.bfloat16, jnp.float32
        dma = pltpu.SemaphoreType.DMA
        return pl.pallas_call(
            functools.partial(block_kernel, chips),
            out_shape=jax.ShapeDtypeStruct(act_in.shape, bf),
            in_specs=[hbm, vmem, vmem, hbm, vmem, vmem, vmem, hbm, vmem, hbm, hbm, vmem],
            out_specs=hbm,
            scratch_shapes=[
                pltpu.VMEM((model, ffn), bf),
                pltpu.VMEM((gate, model), bf),
                pltpu.VMEM((chips, rows, model), bf),
                pltpu.VMEM((rows, model), bf),
                pltpu.VMEM((rows, gate), bf),
                pltpu.VMEM((chips, rows, gate), bf),
                pltpu.VMEM((seq, gate), bf),
                pltpu.VMEM((chips, rows, seq), bf),
                pltpu.VMEM((tiles, rows, span), jnp.int32),
                pltpu.VMEM((rows, gate), bf),
                pltpu.VMEM((chips, rows, model), bf),
                pltpu.VMEM((chips, rows, 128), f32),
                pltpu.VMEM((1, model), f32),
                pltpu.VMEM((1, model), f32),
                pltpu.VMEM((1, ffn), f32),
                pltpu.VMEM((1, gate), f32),
                pltpu.VMEM((1, gate), f32),
                pltpu.VMEM((1, model), f32),
                dma((2,)), dma, dma((chips,)), dma((tiles,)), dma,
                dma((chips,)), dma((chips,)), dma((chips,)), dma((chips,)),
                dma((chips, n_out)), dma((chips, n_out)), dma((n_out,)),
            ],
            compiler_params=pltpu.CompilerParams(collective_id=0, has_side_effects=True,
                                                 vmem_limit_bytes=66 * 1000 * 1000),
            name="gmlp_block",
        )(act_in, ln1_scale, ln1_bias, w_in, b_in, ln2_scale, ln2_bias, w_spatial, b_spatial, causal_mask, w_out, b_out)

    return jax.shard_map(local_block, mesh=mesh, in_specs=(row_spec,) + (P(),) * 11, out_specs=row_spec, check_vma=False)
```

```python
import functools

import jax
import jax.numpy as jnp
from jax import lax
from jax.experimental import pallas as pl
from jax.experimental.pallas import tpu as pltpu
from jax.sharding import PartitionSpec as P

LN_EPS = 1e-6
MESH = pl.DeviceIdType.MESH
GELU_A = 0.7978845608028654
GELU_B = 0.7978845608028654 * 0.044715
CORES = 2
NT = 512
OT = 256
PLANS = [
    [0, 4, 3, 1, 2, 5, 7, 6],
    [0, 4, 3, 1, 2, 7, 5, 6],
    [1, 0, 2, 4, 6, 5, 3, 7],
    [1, 0, 2, 4, 6, 5, 3, 7],
    [2, 1, 3, 0, 7, 5, 6, 4],
    [2, 1, 3, 0, 7, 5, 6, 4],
    [3, 0, 2, 1, 5, 4, 6, 7],
    [3, 2, 0, 1, 4, 6, 5, 7],
]
SENDS = [
    [(1, 0), (3, 0), (2, 0)],
    [(1, 0), (3, 0), (2, 0)],
    [(1, 0), (3, 0), (2, 0)],
    [(1, 0), (3, 0), (2, 0)],
    [(1, 0), (3, 0), (2, 0)],
    [(1, 0), (3, 0), (2, 0)],
    [(1, 0), (3, 0), (2, 0)],
    [(1, 0), (3, 0), (2, 0)],
]


def gelu(a):
    return (0.5 * a) * (1.0 + jnp.tanh(a * (GELU_A + GELU_B * (a * a))))


def norm_rows(src, dst, at, groups, width, scale, shift):
    tiles = [slice(t * 128, (t + 1) * 128) for t in range(width // 128)]
    rows = [pl.ds(pl.multiple_of(at[0] + 32 * r, 32), 32) for r in range(groups)]
    to = [pl.ds(pl.multiple_of(at[1] + 32 * r, 32), 32) for r in range(groups)]

    def total(parts):
        acc = parts[0]
        for p in parts[1:]:
            acc = acc + p
        return jnp.sum(acc, axis=-1, keepdims=True) * (1.0 / width)

    def load(r, t):
        return src[r, t].astype(jnp.float32)

    mean = [total([load(r, t) for t in tiles]) for r in rows]
    inv = []
    for r, m in zip(rows, mean):
        inv.append(lax.rsqrt(total([(load(r, t) - m) * (load(r, t) - m) for t in tiles]) + LN_EPS))
    for r, m, s, d in zip(rows, mean, inv, to):
        for t in tiles:
            dst[d, t] = ((load(r, t) - m) * s * scale[:, t] + shift[:, t]).astype(jnp.bfloat16)


def pick(me, values):
    out = values[-1]
    for d in range(len(values) - 1):
        out = jnp.where(me == d, values[d], out)
    return out


def packed(fields, bits):
    return sum(f << (bits * k) for k, f in enumerate(fields))


def partner_waits(plan, chips):
    seen, waits = set(), []
    for op in plan:
        need = set(range(op - chips + 1)) - seen if op >= chips else set()
        seen |= need
        waits.append(sum(1 << j for j in need))
    assert seen == set(range(chips)) and waits[0] == 0
    return waits[1:]


def block_kernel(chips, x_hbm, ln1s_1d, ln1b_1d, w_in_hbm, b_in_1d, ln2s_1d, ln2b_1d, w_sp_hbm, b_sp_1d, mask_hbm,
                 w_out_hbm, b_out_1d, out_hbm,
                 w_in, w_out, xg, u, v, g, vn, wm, mk, q, o, bs, ln1s, ln1b, b_in, ln2s, ln2b, b_out,
                 w_in_sem, w_out_sem, wm_sem, mk_sem, own_sem, x_send, x_recv, v_send, v_recv, o_send, o_recv, o_loc):
    rows, model = x_hbm.shape[1:]
    gate = w_out.shape[0]
    n_in = gate // NT
    span = CORES * rows
    data = lax.axis_index("data")
    me = lax.axis_index("seq")
    chip = me // CORES
    core = me % CORES

    def device(c):
        return (data, c * CORES + core)

    partner = (data, chip * CORES + (1 - core))

    barrier = pltpu.get_barrier_semaphore()
    for d in range(1, chips):
        pl.semaphore_signal(barrier, inc=1, device_id=device((chip + d) % chips), device_id_type=MESH)
    pl.semaphore_signal(barrier, inc=1, device_id=partner, device_id_type=MESH)

    own_copy = pltpu.make_async_copy(x_hbm.at[chip], xg.at[chip], own_sem)
    own_copy.start()
    w_in_copies = []
    for n in range(2):
        cols = pl.ds(gate * (1 - n), gate)
        w_in_copies.append(pltpu.make_async_copy(w_in_hbm.at[:, cols], w_in.at[:, cols], w_in_sem.at[n]))
    w_in_copies[0].start()
    for src, dst in ((ln1s_1d, ln1s), (ln1b_1d, ln1b), (b_in_1d, b_in), (ln2s_1d, ln2s), (ln2b_1d, ln2b),
                     (b_out_1d, b_out)):
        dst[...] = src[...].reshape(1, -1)

    pl.semaphore_wait(barrier, chips)

    def x_copy(d):
        to = (chip + d) % chips
        return pltpu.make_async_remote_copy(
            src_ref=x_hbm.at[to], dst_ref=xg.at[chip], send_sem=x_send.at[d], recv_sem=x_recv.at[d],
            device_id=device(to), device_id_type=MESH)

    sends = pick(me, [packed([d + (late << 2) for d, late in p], 3) for p in SENDS])

    def start_sends(late):
        for slot in range(chips - 1):
            field = lax.shift_right_logical(sends, 3 * slot) % 8

            @pl.when(field // 4 == late)
            def _(field=field):
                x_copy(field % 4).start()

    start_sends(0)

    w_in_copies[1].start()
    wm_copies, mk_copies = [], []
    t = 0
    for i in range(chips):
        r = pl.ds(pl.multiple_of((CORES * i + core) * rows, rows), rows)
        cp = pltpu.make_async_copy(w_sp_hbm.at[r, pl.ds(0, span * (i + 1))], wm.at[i, :, pl.ds(0, span * (i + 1))],
                                   wm_sem.at[i])
        cp.start()
        wm_copies.append(cp)
        for j in range(i + 1):
            cp = pltpu.make_async_copy(mask_hbm.at[r, pl.ds(span * j, span)], mk.at[t], mk_sem.at[t])
            cp.start()
            mk_copies.append(cp)
            t += 1
    w_out_copy = pltpu.make_async_copy(w_out_hbm, w_out, w_out_sem)
    w_out_copy.start()

    def vn_copy(j):
        r = pl.ds(pl.multiple_of((CORES * j + core) * rows, rows), rows)
        return pltpu.make_async_remote_copy(
            src_ref=vn.at[r], dst_ref=vn.at[r], send_sem=v_send.at[j], recv_sem=v_recv.at[j],
            device_id=partner, device_id_type=MESH)

    def hidden(k, j):
        @pl.when(k == 0)
        def _():
            own_copy.wait()
            w_in_copies[0].wait()

        @pl.when(k > 0)
        def _():
            x_copy((chip - j + chips) % chips).wait_recv()

        norm_rows(xg.at[j], u, (0, 0), rows // 32, model, ln1s, ln1b)

        def half(dst, base, n):
            cols = slice(n * NT, (n + 1) * NT)
            wcols = slice(base + n * NT, base + (n + 1) * NT)
            a = jnp.dot(u[...], w_in[:, wcols], preferred_element_type=jnp.float32) + b_in[:, wcols]
            dst[:, cols] = gelu(a).astype(jnp.bfloat16)

        for n in range(n_in):
            half(v, gate, n)

        own_rows = (CORES * j + core) * rows

        @pl.loop(0, 2)
        def _(r):
            norm_rows(v, vn, (r * 128, own_rows + r * 128), 4, gate, ln2s, ln2b)

        @pl.when(k == 0)
        def _():
            w_in_copies[1].wait()

        half(g.at[j], 0, 0)
        vn_copy(j).start()
        for n in range(1, n_in):
            half(g.at[j], 0, n)

    def mask_weights():
        for cp in wm_copies + mk_copies:
            cp.wait()
        t = 0
        for i in range(chips):
            for j in range(i + 1):
                cols = pl.ds(span * j, span)

                @pl.loop(0, rows // 32)
                def _(r, i=i, t=t, cols=cols):
                    rr = pl.ds(pl.multiple_of(r * 32, 32), 32)
                    w = wm[i, rr, cols].astype(jnp.float32)
                    wm[i, rr, cols] = jnp.where(mk[t, rr, :] > 0, w, 0.0).astype(jnp.bfloat16)

                t += 1
            row = b_sp_1d[pl.ds(pl.multiple_of((CORES * i + core) * rows, rows), rows)].reshape(1, rows)
            bs[i, :, :] = jnp.transpose(jnp.broadcast_to(row, (128, rows)))

    cuts = [(0, 768), (768, model)] if model > 768 else [(0, model)]

    def o_copy(i, n, recv):
        cols = pl.ds(cuts[n][0], cuts[n][1] - cuts[n][0])
        return pltpu.make_async_remote_copy(
            src_ref=o.at[i, :, cols], dst_ref=out_hbm.at[chip, :, cols], send_sem=o_send.at[i, n],
            recv_sem=o_recv.at[recv, n], device_id=device(i), device_id_type=MESH)

    def o_local(n):
        cols = pl.ds(cuts[n][0], cuts[n][1] - cuts[n][0])
        return pltpu.make_async_copy(o.at[chip, :, cols], out_hbm.at[chip, :, cols], o_loc.at[n])

    def mix(i, waits):
        for j in range(chips):
            @pl.when(lax.shift_right_logical(waits, j) % 2 == 1)
            def _(j=j):
                vn_copy(j).wait_recv()

        for s in range(chips):
            @pl.when(i == s)
            def _(s=s):
                depth = span * (s + 1)
                for n in range(n_in):
                    cols = slice(n * NT, (n + 1) * NT)
                    acc = jnp.dot(wm[s, :, :depth], vn[:depth, cols], preferred_element_type=jnp.float32)
                    sp = (acc + bs[s, :, 0:1]).astype(jnp.bfloat16).astype(jnp.float32)
                    q[:, cols] = (g[s, :, cols].astype(jnp.float32) * sp).astype(jnp.bfloat16)

        for n, (lo, hi) in enumerate(cuts):
            for c in range(lo, hi, OT):
                cols = slice(c, c + OT)
                y = jnp.dot(q[...], w_out[:, cols], preferred_element_type=jnp.float32) + b_out[:, cols]
                o[i, :, cols] = (xg[i, :, cols].astype(jnp.float32) + y).astype(jnp.bfloat16)

            @pl.when(i != chip)
            def _(n=n):
                o_copy(i, n, chip).start()

            @pl.when(i == chip)
            def _(n=n):
                o_local(n).start()

    plan = pick(me, [packed(p, 3) for p in PLANS])
    plan_waits = pick(me, [packed(partner_waits(p, chips), chips) for p in PLANS])

    @pl.loop(0, 2 * chips)
    def _(k):
        op = lax.shift_right_logical(plan, 3 * k) % 8

        @pl.when(op < chips)
        def _():
            hidden(k, op)

        @pl.when(k == 0)
        def _():
            start_sends(1)
            mask_weights()
            w_out_copy.wait()

        @pl.when(op >= chips)
        def _():
            mix(op - chips, lax.shift_right_logical(plan_waits, chips * (k - 1)) % (1 << chips))

    for d in range(1, chips):
        x_copy(d).wait_send()
        src = (chip - d + chips) % chips
        for n in range(len(cuts)):
            o_copy(src, n, chip).wait_send()
            o_copy(src, n, src).wait_recv()
    for n in range(len(cuts)):
        o_local(n).wait()
    for j in range(chips):
        vn_copy(j).wait_send()


def solution(mesh):
    row_spec = P('data', 'seq', None)
    chips = mesh.shape['seq'] // CORES

    def local_block(act_in, ln1_scale, ln1_bias, w_in, b_in, ln2_scale, ln2_bias, w_spatial, b_spatial, causal_mask, w_out, b_out):
        batch, rows, model = act_in.shape
        ffn = w_in.shape[1]
        gate = w_out.shape[0]
        seq = w_spatial.shape[0]
        span = CORES * rows
        assert batch == chips and span * chips == seq
        n_out = 2 if model > 768 else 1
        assert chips == 4 and len(PLANS) == len(SENDS) == CORES * chips
        tiles = chips * (chips + 1) // 2
        hbm = pl.BlockSpec(memory_space=pl.ANY)
        vmem = pl.BlockSpec(memory_space=pltpu.VMEM)
        bf, f32 = jnp.bfloat16, jnp.float32
        dma = pltpu.SemaphoreType.DMA
        return pl.pallas_call(
            functools.partial(block_kernel, chips),
            out_shape=pltpu.VMEM(act_in.shape, bf),
            in_specs=[hbm, vmem, vmem, hbm, vmem, vmem, vmem, hbm, vmem, hbm, hbm, vmem],
            out_specs=hbm,
            scratch_shapes=[
                pltpu.VMEM((model, ffn), bf),
                pltpu.VMEM((gate, model), bf),
                pltpu.VMEM((chips, rows, model), bf),
                pltpu.VMEM((rows, model), bf),
                pltpu.VMEM((rows, gate), bf),
                pltpu.VMEM((chips, rows, gate), bf),
                pltpu.VMEM((seq, gate), bf),
                pltpu.VMEM((chips, rows, seq), bf),
                pltpu.VMEM((tiles, rows, span), jnp.int32),
                pltpu.VMEM((rows, gate), bf),
                pltpu.VMEM((chips, rows, model), bf),
                pltpu.VMEM((chips, rows, 128), f32),
                pltpu.VMEM((1, model), f32),
                pltpu.VMEM((1, model), f32),
                pltpu.VMEM((1, ffn), f32),
                pltpu.VMEM((1, gate), f32),
                pltpu.VMEM((1, gate), f32),
                pltpu.VMEM((1, model), f32),
                dma((2,)), dma, dma((chips,)), dma((tiles,)), dma,
                dma((chips,)), dma((chips,)), dma((chips,)), dma((chips,)),
                dma((chips, n_out)), dma((chips, n_out)), dma((n_out,)),
            ],
            compiler_params=pltpu.CompilerParams(collective_id=0, has_side_effects=True,
                                                 vmem_limit_bytes=62 * 1000 * 1000),
            name="gmlp_block",
        )(act_in, ln1_scale, ln1_bias, w_in, b_in, ln2_scale, ln2_bias, w_spatial, b_spatial, causal_mask, w_out, b_out)

    return jax.shard_map(local_block, mesh=mesh, in_specs=(row_spec,) + (P(),) * 11, out_specs=row_spec, check_vma=False)
```

```python
import functools

import jax
import jax.numpy as jnp
from jax import lax
from jax.experimental import pallas as pl
from jax.experimental.pallas import tpu as pltpu
from jax.sharding import PartitionSpec as P

LN_EPS = 1e-6
MESH = pl.DeviceIdType.MESH
GELU_A = 0.7978845608028654
GELU_B = 0.7978845608028654 * 0.044715
CORES = 2
HT = 256
NT = 512
OT = 256
PLANS = [
    [0, 1, 3, 2, 6, 5, 7, 4],
    [0, 1, 3, 2, 6, 5, 7, 4],
    [1, 0, 2, 3, 7, 6, 4, 5],
    [1, 0, 2, 3, 7, 6, 4, 5],
    [2, 1, 0, 4, 3, 5, 7, 6],
    [2, 1, 0, 4, 3, 5, 7, 6],
    [3, 0, 1, 5, 2, 6, 4, 7],
    [3, 0, 1, 5, 2, 6, 4, 7],
]
SENDS = [
    [(1, 0), (3, 0), (2, 2)],
    [(3, 0), (1, 1), (2, 2)],
    [(3, 0), (1, 0), (2, 1)],
    [(1, 0), (3, 1), (2, 2)],
    [(3, 0), (1, 0), (2, 1)],
    [(1, 0), (3, 1), (2, 2)],
    [(3, 0), (1, 0), (2, 0)],
    [(3, 0), (1, 1), (2, 2)],
]


def gelu(a):
    return (0.5 * a) * (1.0 + jnp.tanh(a * (GELU_A + GELU_B * (a * a))))


def norm_rows(src, dst, at, groups, width, scale, shift):
    tiles = [slice(t * 128, (t + 1) * 128) for t in range(width // 128)]
    rows = [pl.ds(pl.multiple_of(at[0] + 32 * r, 32), 32) for r in range(groups)]
    to = [pl.ds(pl.multiple_of(at[1] + 32 * r, 32), 32) for r in range(groups)]

    def total(parts):
        acc = parts[0]
        for p in parts[1:]:
            acc = acc + p
        return jnp.sum(acc, axis=-1, keepdims=True) * (1.0 / width)

    def load(r, t):
        return src[r, t].astype(jnp.float32)

    mean = [total([load(r, t) for t in tiles]) for r in rows]
    inv = []
    for r, m in zip(rows, mean):
        inv.append(lax.rsqrt(total([(load(r, t) - m) * (load(r, t) - m) for t in tiles]) + LN_EPS))
    for r, m, s, d in zip(rows, mean, inv, to):
        for t in tiles:
            dst[d, t] = ((load(r, t) - m) * s * scale[:, t] + shift[:, t]).astype(jnp.bfloat16)


def pick(me, values):
    out = values[-1]
    for d in range(len(values) - 1):
        out = jnp.where(me == d, values[d], out)
    return out


def packed(fields, bits):
    return sum(f << (bits * k) for k, f in enumerate(fields))


def partner_waits(plan, chips, core):
    seen, waits = set(), []
    for k, op in enumerate(plan):
        need = set(range(op - chips + core)) - seen if op >= chips else set()
        if k == len(plan) - 1:
            need = set(range(chips)) - seen
        seen |= need
        waits.append(sum(1 << j for j in need))
    assert waits[0] == 0
    return waits[1:]


def block_kernel(chips, x_hbm, ln1s_1d, ln1b_1d, w_in_hbm, b_in_1d, ln2s_1d, ln2b_1d, w_sp_hbm, b_sp_1d, mask_hbm,
                 w_out_hbm, b_out_1d, out_hbm,
                 w_in, w_out, xg, xs, u, v, g, vn, wm, mk, q, o, bs, ln1s, ln1b, b_in, ln2s, ln2b, b_out,
                 w_in_sem, w_out_sem, wm_sem, mk_sem, own_sem, xs_sem, x_send, x_recv, v_send, v_recv, o_send, o_recv, o_loc):
    rows, model = x_hbm.shape[1:]
    gate = w_out.shape[0]
    n_in = gate // NT
    span = CORES * rows
    data = lax.axis_index("data")
    me = lax.axis_index("seq")
    chip = me // CORES
    core = me % CORES

    def device(c):
        return (data, c * CORES + core)

    partner = (data, chip * CORES + (1 - core))

    barrier = pltpu.get_barrier_semaphore()
    for d in range(1, chips):
        pl.semaphore_signal(barrier, inc=1, device_id=device((chip + d) % chips), device_id_type=MESH)
    pl.semaphore_signal(barrier, inc=1, device_id=partner, device_id_type=MESH)

    own_copy = pltpu.make_async_copy(x_hbm.at[chip], xg.at[chip], own_sem)
    own_copy.start()
    w_in_copies = []
    for n in range(2):
        cols = pl.ds(gate * (1 - n), gate)
        w_in_copies.append(pltpu.make_async_copy(w_in_hbm.at[:, cols], w_in.at[:, cols], w_in_sem.at[n]))
    w_in_copies[0].start()
    for src, dst in ((ln1s_1d, ln1s), (ln1b_1d, ln1b), (b_in_1d, b_in), (ln2s_1d, ln2s), (ln2b_1d, ln2b),
                     (b_out_1d, b_out)):
        dst[...] = src[...].reshape(1, -1)

    pl.semaphore_wait(barrier, chips)

    def x_copy(d, src):
        to = (chip + d) % chips
        return pltpu.make_async_remote_copy(
            src_ref=src.at[to], dst_ref=xg.at[chip], send_sem=x_send.at[d], recv_sem=x_recv.at[d],
            device_id=device(to), device_id_type=MESH)

    sends = pick(me, [packed([d + (stage << 2) for d, stage in p], 4) for p in SENDS])

    def start_sends(stage):
        for slot in range(chips - 1):
            field = lax.shift_right_logical(sends, 4 * slot) % 16

            @pl.when(field // 4 == (0 if stage is None else stage))
            def _(field=field):
                x_copy(field % 4, x_hbm if stage is None else xs).start()

    start_sends(None)
    xs_copy = pltpu.make_async_copy(x_hbm, xs, xs_sem)
    xs_copy.start()
    w_in_copies[1].start()

    wm_copies, mk_copies = [], []
    t = 0
    for i in range(chips):
        r = pl.ds(pl.multiple_of((CORES * i + core) * rows, rows), rows)
        cp = pltpu.make_async_copy(w_sp_hbm.at[r, pl.ds(0, span * (i + 1))], wm.at[i, :, pl.ds(0, span * (i + 1))],
                                   wm_sem.at[i])
        cp.start()
        wm_copies.append(cp)
        for j in range(i + 1):
            cp = pltpu.make_async_copy(mask_hbm.at[r, pl.ds(span * j, span)], mk.at[t], mk_sem.at[t])
            cp.start()
            mk_copies.append(cp)
            t += 1
    w_out_copy = pltpu.make_async_copy(w_out_hbm, w_out, w_out_sem)
    w_out_copy.start()

    def vn_copy(j):
        r = pl.ds(pl.multiple_of((CORES * j + core) * rows, rows), rows)
        return pltpu.make_async_remote_copy(
            src_ref=vn.at[r], dst_ref=vn.at[r], send_sem=v_send.at[j], recv_sem=v_recv.at[j],
            device_id=partner, device_id_type=MESH)

    def hidden(k, h, j):
        @pl.when(k == 0)
        def _():
            own_copy.wait()
            w_in_copies[0].wait()

        @pl.when(k > 0)
        def _():
            x_copy((chip - j + chips) % chips, xs).wait_recv()

        norm_rows(xg.at[j], u, (0, 0), rows // 32, model, ln1s, ln1b)

        def half(dst, base, first, last):
            def finish(n, a):
                a = a + b_in[:, base + n * HT:base + (n + 1) * HT]
                dst[:, n * HT:(n + 1) * HT] = gelu(a).astype(jnp.bfloat16)

            held = None
            for n in range(first, last):
                a = jnp.dot(u[...], w_in[:, base + n * HT:base + (n + 1) * HT], preferred_element_type=jnp.float32)
                if held is not None:
                    finish(n - 1, held)
                held = a
            finish(last - 1, held)

        half(v, gate, 0, gate // HT)

        own_rows = (CORES * j + core) * rows

        @pl.when(k == 0)
        def _():
            w_in_copies[1].wait()
            xs_copy.wait()

        norm_rows(v, vn, (0, own_rows), rows // 32, gate, ln2s, ln2b)
        half(g.at[j], 0, 0, 5)
        vn_copy(j).start()
        start_sends(h + 1)
        half(g.at[j], 0, 5, gate // HT)

    def mask_weights():
        for cp in wm_copies + mk_copies:
            cp.wait()
        t = 0
        for i in range(chips):
            for j in range(i + 1):
                cols = pl.ds(span * j, span)

                @pl.loop(0, rows // 32)
                def _(r, i=i, t=t, cols=cols):
                    rr = pl.ds(pl.multiple_of(r * 32, 32), 32)
                    w = wm[i, rr, cols].astype(jnp.float32)
                    wm[i, rr, cols] = jnp.where(mk[t, rr, :] > 0, w, 0.0).astype(jnp.bfloat16)

                t += 1
            row = b_sp_1d[pl.ds(pl.multiple_of((CORES * i + core) * rows, rows), rows)].reshape(1, rows)
            bs[i, :, :] = jnp.transpose(jnp.broadcast_to(row, (128, rows)))

    cuts = [(0, 768), (768, model)] if model > 768 else [(0, model)]

    def o_copy(i, n, recv):
        cols = pl.ds(cuts[n][0], cuts[n][1] - cuts[n][0])
        return pltpu.make_async_remote_copy(
            src_ref=o.at[i, :, cols], dst_ref=out_hbm.at[chip, :, cols], send_sem=o_send.at[i, n],
            recv_sem=o_recv.at[recv, n], device_id=device(i), device_id_type=MESH)

    def o_local(n):
        cols = pl.ds(cuts[n][0], cuts[n][1] - cuts[n][0])
        return pltpu.make_async_copy(o.at[chip, :, cols], out_hbm.at[chip, :, cols], o_loc.at[n])

    def mix(i, waits):
        for j in range(chips):
            @pl.when(lax.shift_right_logical(waits, j) % 2 == 1)
            def _(j=j):
                vn_copy(j).wait_recv()

        for s, c in [(s, c) for s in range(chips) for c in range(CORES)]:
            @pl.when((i == s) & (core == c))
            def _(s=s, depth=span * s + rows * (c + 1)):
                for n in range(n_in):
                    cols = slice(n * NT, (n + 1) * NT)
                    acc = jnp.dot(wm[s, :, :depth], vn[:depth, cols], preferred_element_type=jnp.float32)
                    sp = (acc + bs[s, :, 0:1]).astype(jnp.bfloat16).astype(jnp.float32)
                    q[:, cols] = (g[s, :, cols].astype(jnp.float32) * sp).astype(jnp.bfloat16)

        for n, (lo, hi) in enumerate(cuts):
            for c in range(lo, hi, OT):
                cols = slice(c, c + OT)
                y = jnp.dot(q[...], w_out[:, cols], preferred_element_type=jnp.float32) + b_out[:, cols]
                o[i, :, cols] = (xg[i, :, cols].astype(jnp.float32) + y).astype(jnp.bfloat16)

            @pl.when(i != chip)
            def _(n=n):
                o_copy(i, n, chip).start()

            @pl.when(i == chip)
            def _(n=n):
                o_local(n).start()

    plan = pick(me, [packed(p, 3) for p in PLANS])
    counts = pick(me, [packed([sum(o < chips for o in p[:k]) % 4 for k in range(len(p))], 2) for p in PLANS])
    plan_waits = pick(me, [packed(partner_waits(p, chips, d % CORES), chips) for d, p in enumerate(PLANS)])

    @pl.loop(0, 2 * chips)
    def _(k):
        op = lax.shift_right_logical(plan, 3 * k) % 8

        @pl.when(op < chips)
        def _():
            hidden(k, lax.shift_right_logical(counts, 2 * k) % 4, op)

        @pl.when(k == 0)
        def _():
            mask_weights()
            w_out_copy.wait()

        @pl.when(op >= chips)
        def _():
            mix(op - chips, lax.shift_right_logical(plan_waits, chips * (k - 1)) % (1 << chips))

    for d in range(1, chips):
        x_copy(d, xs).wait_send()
        src = (chip - d + chips) % chips
        for n in range(len(cuts)):
            o_copy(src, n, chip).wait_send()
            o_copy(src, n, src).wait_recv()
    for n in range(len(cuts)):
        o_local(n).wait()
    for j in range(chips):
        vn_copy(j).wait_send()


def solution(mesh):
    row_spec = P('data', 'seq', None)
    chips = mesh.shape['seq'] // CORES

    def local_block(act_in, ln1_scale, ln1_bias, w_in, b_in, ln2_scale, ln2_bias, w_spatial, b_spatial, causal_mask, w_out, b_out):
        batch, rows, model = act_in.shape
        ffn = w_in.shape[1]
        gate = w_out.shape[0]
        seq = w_spatial.shape[0]
        span = CORES * rows
        assert batch == chips and span * chips == seq
        n_out = 2 if model > 768 else 1
        assert chips == 4 and len(PLANS) == len(SENDS) == CORES * chips
        tiles = chips * (chips + 1) // 2
        hbm = pl.BlockSpec(memory_space=pl.ANY)
        vmem = pl.BlockSpec(memory_space=pltpu.VMEM)
        bf, f32 = jnp.bfloat16, jnp.float32
        dma = pltpu.SemaphoreType.DMA
        return pl.pallas_call(
            functools.partial(block_kernel, chips),
            out_shape=pltpu.VMEM(act_in.shape, bf),
            in_specs=[hbm, vmem, vmem, hbm, vmem, vmem, vmem, hbm, vmem, hbm, hbm, vmem],
            out_specs=hbm,
            scratch_shapes=[
                pltpu.VMEM((model, ffn), bf),
                pltpu.VMEM((gate, model), bf),
                pltpu.VMEM((chips, rows, model), bf),
                pltpu.VMEM((chips, rows, model), bf),
                pltpu.VMEM((rows, model), bf),
                pltpu.VMEM((rows, gate), bf),
                pltpu.VMEM((chips, rows, gate), bf),
                pltpu.VMEM((seq, gate), bf),
                pltpu.VMEM((chips, rows, seq), bf),
                pltpu.VMEM((tiles, rows, span), jnp.int32),
                pltpu.VMEM((rows, gate), bf),
                pltpu.VMEM((chips, rows, model), bf),
                pltpu.VMEM((chips, rows, 128), f32),
                pltpu.VMEM((1, model), f32),
                pltpu.VMEM((1, model), f32),
                pltpu.VMEM((1, ffn), f32),
                pltpu.VMEM((1, gate), f32),
                pltpu.VMEM((1, gate), f32),
                pltpu.VMEM((1, model), f32),
                dma((2,)), dma, dma((chips,)), dma((tiles,)), dma, dma,
                dma((chips,)), dma((chips,)), dma((chips,)), dma((chips,)),
                dma((chips, n_out)), dma((chips, n_out)), dma((n_out,)),
            ],
            compiler_params=pltpu.CompilerParams(collective_id=0, has_side_effects=True,
                                                 vmem_limit_bytes=62 * 1000 * 1000),
            name="gmlp_block",
        )(act_in, ln1_scale, ln1_bias, w_in, b_in, ln2_scale, ln2_bias, w_spatial, b_spatial, causal_mask, w_out, b_out)

    return jax.shard_map(local_block, mesh=mesh, in_specs=(row_spec,) + (P(),) * 11, out_specs=row_spec, check_vma=False)
```

```python
import functools

import jax
import jax.numpy as jnp
from jax import lax
from jax.experimental import pallas as pl
from jax.experimental.pallas import tpu as pltpu
from jax.sharding import PartitionSpec as P

LN_EPS = 1e-6
MESH = pl.DeviceIdType.MESH
GELU_A = 0.7978845608028654
GELU_B = 0.7978845608028654 * 0.044715
CORES = 2
HT = 256
NT = 512
OT = 256
PLANS = [
    [0, 1, 4, 2, 6, 3, 7, 5],
    [0, 1, 4, 2, 6, 3, 7, 5],
    [1, 2, 0, 3, 7, 6, 4, 5],
    [1, 2, 0, 3, 7, 6, 4, 5],
    [2, 1, 0, 4, 3, 7, 5, 6],
    [2, 1, 0, 4, 3, 7, 5, 6],
    [3, 0, 1, 5, 2, 4, 6, 7],
    [3, 0, 1, 5, 2, 4, 6, 7],
]
SENDS = [
    [(3, 0), (1, 1), (2, 2)],
    [(1, 0), (3, 1), (2, 2)],
    [(3, 0), (1, 0), (2, 2)],
    [(1, 0), (3, 1), (2, 2)],
    [(2, 0), (3, 0), (1, 1)],
    [(2, 0), (3, 1), (1, 2)],
    [(3, 0), (1, 2), (2, 2)],
    [(3, 0), (2, 2), (1, 2)],
]


def gelu(a):
    return (0.5 * a) * (1.0 + jnp.tanh(a * (GELU_A + GELU_B * (a * a))))


def norm_rows(src, dst, at, groups, width, scale, shift):
    tiles = [slice(t * 128, (t + 1) * 128) for t in range(width // 128)]
    rows = [pl.ds(pl.multiple_of(at[0] + 32 * r, 32), 32) for r in range(groups)]
    to = [pl.ds(pl.multiple_of(at[1] + 32 * r, 32), 32) for r in range(groups)]

    def total(parts):
        acc = parts[0]
        for p in parts[1:]:
            acc = acc + p
        return jnp.sum(acc, axis=-1, keepdims=True) * (1.0 / width)

    def load(r, t):
        return src[r, t].astype(jnp.float32)

    mean = [total([load(r, t) for t in tiles]) for r in rows]
    inv = []
    for r, m in zip(rows, mean):
        inv.append(lax.rsqrt(total([(load(r, t) - m) * (load(r, t) - m) for t in tiles]) + LN_EPS))
    for r, m, s, d in zip(rows, mean, inv, to):
        for t in tiles:
            dst[d, t] = ((load(r, t) - m) * s * scale[:, t] + shift[:, t]).astype(jnp.bfloat16)


def pick(me, values):
    out = values[-1]
    for d in range(len(values) - 1):
        out = jnp.where(me == d, values[d], out)
    return out


def packed(fields, bits):
    return sum(f << (bits * k) for k, f in enumerate(fields))


def partner_waits(plan, chips, core):
    seen, waits = set(), []
    for k, op in enumerate(plan):
        need = set(range(op - chips + core)) - seen if op >= chips else set()
        if k == len(plan) - 1:
            need = set(range(chips)) - seen
        seen |= need
        waits.append(sum(1 << j for j in need))
    assert waits[0] == 0
    return waits[1:]


def block_kernel(chips, x_hbm, ln1s_1d, ln1b_1d, w_in_hbm, b_in_1d, ln2s_1d, ln2b_1d, w_sp_hbm, b_sp_1d, mask_hbm,
                 w_out_hbm, b_out_1d, out_hbm,
                 w_in, w_out, xg, xs, u, v, g, vn, wm, mk, q, o, bs, ln1s, ln1b, b_in, ln2s, ln2b, b_out,
                 w_in_sem, w_out_sem, wm_sem, mk_sem, own_sem, xs_sem, x_send, x_recv, v_send, v_recv, o_send, o_recv, o_loc):
    rows, model = x_hbm.shape[1:]
    gate = w_out.shape[0]
    n_in = gate // NT
    span = CORES * rows
    data = lax.axis_index("data")
    me = lax.axis_index("seq")
    chip = me // CORES
    core = me % CORES

    def device(c):
        return (data, c * CORES + core)

    partner = (data, chip * CORES + (1 - core))

    barrier = pltpu.get_barrier_semaphore()
    for d in range(1, chips):
        pl.semaphore_signal(barrier, inc=1, device_id=device((chip + d) % chips), device_id_type=MESH)
    pl.semaphore_signal(barrier, inc=1, device_id=partner, device_id_type=MESH)

    own_copy = pltpu.make_async_copy(x_hbm.at[chip], xg.at[chip], own_sem)
    own_copy.start()
    w_in_copies = []
    for n in range(2):
        cols = pl.ds(gate * (1 - n), gate)
        w_in_copies.append(pltpu.make_async_copy(w_in_hbm.at[:, cols], w_in.at[:, cols], w_in_sem.at[n]))
    w_in_copies[0].start()
    for src, dst in ((ln1s_1d, ln1s), (ln1b_1d, ln1b), (b_in_1d, b_in), (ln2s_1d, ln2s), (ln2b_1d, ln2b),
                     (b_out_1d, b_out)):
        dst[...] = src[...].reshape(1, -1)

    pl.semaphore_wait(barrier, chips)

    def x_copy(d, src):
        to = (chip + d) % chips
        return pltpu.make_async_remote_copy(
            src_ref=src.at[to], dst_ref=xg.at[chip], send_sem=x_send.at[d], recv_sem=x_recv.at[d],
            device_id=device(to), device_id_type=MESH)

    sends = pick(me, [packed([d + (stage << 2) for d, stage in p], 4) for p in SENDS])

    def start_sends(stage, src):
        for slot in range(chips - 1):
            field = lax.shift_right_logical(sends, 4 * slot) % 16

            @pl.when(field // 4 == stage)
            def _(field=field):
                x_copy(field % 4, src).start()

    start_sends(0, x_hbm)
    w_in_copies[1].start()

    wm_copies, mk_copies = [], []
    t = 0
    for i in range(chips):
        r = pl.ds(pl.multiple_of((CORES * i + core) * rows, rows), rows)
        cp = pltpu.make_async_copy(w_sp_hbm.at[r, pl.ds(0, span * (i + 1))], wm.at[i, :, pl.ds(0, span * (i + 1))],
                                   wm_sem.at[i])
        cp.start()
        wm_copies.append(cp)
        for j in range(i + 1):
            cp = pltpu.make_async_copy(mask_hbm.at[r, pl.ds(span * j, span)], mk.at[t], mk_sem.at[t])
            cp.start()
            mk_copies.append(cp)
            t += 1
    w_out_copy = pltpu.make_async_copy(w_out_hbm, w_out, w_out_sem)
    w_out_copy.start()
    xs_copy = pltpu.make_async_copy(x_hbm, xs, xs_sem)
    xs_copy.start()

    def vn_copy(j):
        r = pl.ds(pl.multiple_of((CORES * j + core) * rows, rows), rows)
        return pltpu.make_async_remote_copy(
            src_ref=vn.at[r], dst_ref=vn.at[r], send_sem=v_send.at[j], recv_sem=v_recv.at[j],
            device_id=partner, device_id_type=MESH)

    def hidden(k, h, j):
        @pl.when(k == 0)
        def _():
            own_copy.wait()
            w_in_copies[0].wait()

        @pl.when(k > 0)
        def _():
            x_copy((chip - j + chips) % chips, xs).wait_recv()

        norm_rows(xg.at[j], u, (0, 0), rows // 32, model, ln1s, ln1b)

        def half(dst, base, first, last):
            def finish(n, a):
                a = a + b_in[:, base + n * HT:base + (n + 1) * HT]
                dst[:, n * HT:(n + 1) * HT] = gelu(a).astype(jnp.bfloat16)

            held = None
            for n in range(first, last):
                a = jnp.dot(u[...], w_in[:, base + n * HT:base + (n + 1) * HT], preferred_element_type=jnp.float32)
                if held is not None:
                    finish(n - 1, held)
                held = a
            finish(last - 1, held)

        half(v, gate, 0, gate // HT)

        own_rows = (CORES * j + core) * rows

        @pl.when(k == 0)
        def _():
            w_in_copies[1].wait()

        norm_rows(v, vn, (0, own_rows), rows // 32, gate, ln2s, ln2b)
        half(g.at[j], 0, 0, 5)
        vn_copy(j).start()

        @pl.when(h == 0)
        def _():
            start_sends(1, x_hbm)

        @pl.when(h == 1)
        def _():
            xs_copy.wait()

        @pl.when(h > 0)
        def _():
            start_sends(h + 1, xs)

        half(g.at[j], 0, 5, gate // HT)

    def mask_weights():
        for cp in wm_copies + mk_copies:
            cp.wait()
        t = 0
        for i in range(chips):
            for j in range(i + 1):
                cols = pl.ds(span * j, span)

                @pl.loop(0, rows // 32)
                def _(r, i=i, t=t, cols=cols):
                    rr = pl.ds(pl.multiple_of(r * 32, 32), 32)
                    w = wm[i, rr, cols].astype(jnp.float32)
                    wm[i, rr, cols] = jnp.where(mk[t, rr, :] > 0, w, 0.0).astype(jnp.bfloat16)

                t += 1
            row = b_sp_1d[pl.ds(pl.multiple_of((CORES * i + core) * rows, rows), rows)].reshape(1, rows)
            bs[i, :, :] = jnp.transpose(jnp.broadcast_to(row, (128, rows)))

    cuts = [(0, 768), (768, model)] if model > 768 else [(0, model)]

    def o_copy(i, n, recv):
        cols = pl.ds(cuts[n][0], cuts[n][1] - cuts[n][0])
        return pltpu.make_async_remote_copy(
            src_ref=o.at[i, :, cols], dst_ref=out_hbm.at[chip, :, cols], send_sem=o_send.at[i, n],
            recv_sem=o_recv.at[recv, n], device_id=device(i), device_id_type=MESH)

    def o_local(n):
        cols = pl.ds(cuts[n][0], cuts[n][1] - cuts[n][0])
        return pltpu.make_async_copy(o.at[chip, :, cols], out_hbm.at[chip, :, cols], o_loc.at[n])

    def mix(i, waits):
        for j in range(chips):
            @pl.when(lax.shift_right_logical(waits, j) % 2 == 1)
            def _(j=j):
                vn_copy(j).wait_recv()

        for s, c in [(s, c) for s in range(chips) for c in range(CORES)]:
            @pl.when((i == s) & (core == c))
            def _(s=s, depth=span * s + rows * (c + 1)):
                for n in range(n_in):
                    cols = slice(n * NT, (n + 1) * NT)
                    acc = jnp.dot(wm[s, :, :depth], vn[:depth, cols], preferred_element_type=jnp.float32)
                    sp = (acc + bs[s, :, 0:1]).astype(jnp.bfloat16).astype(jnp.float32)
                    q[:, cols] = (g[s, :, cols].astype(jnp.float32) * sp).astype(jnp.bfloat16)

        for n, (lo, hi) in enumerate(cuts):
            for c in range(lo, hi, OT):
                cols = slice(c, c + OT)
                y = jnp.dot(q[...], w_out[:, cols], preferred_element_type=jnp.float32) + b_out[:, cols]
                o[i, :, cols] = (xg[i, :, cols].astype(jnp.float32) + y).astype(jnp.bfloat16)

            @pl.when(i != chip)
            def _(n=n):
                o_copy(i, n, chip).start()

            @pl.when(i == chip)
            def _(n=n):
                o_local(n).start()

    plan = pick(me, [packed(p, 3) for p in PLANS])
    counts = pick(me, [packed([sum(o < chips for o in p[:k]) % 4 for k in range(len(p))], 2) for p in PLANS])
    plan_waits = pick(me, [packed(partner_waits(p, chips, d % CORES), chips) for d, p in enumerate(PLANS)])

    @pl.loop(0, 2 * chips)
    def _(k):
        op = lax.shift_right_logical(plan, 3 * k) % 8

        @pl.when(op < chips)
        def _():
            hidden(k, lax.shift_right_logical(counts, 2 * k) % 4, op)

        @pl.when(k == 0)
        def _():
            mask_weights()
            w_out_copy.wait()

        @pl.when(op >= chips)
        def _():
            mix(op - chips, lax.shift_right_logical(plan_waits, chips * (k - 1)) % (1 << chips))

    for d in range(1, chips):
        x_copy(d, xs).wait_send()
        src = (chip - d + chips) % chips
        for n in range(len(cuts)):
            o_copy(src, n, chip).wait_send()
            o_copy(src, n, src).wait_recv()
    for n in range(len(cuts)):
        o_local(n).wait()
    for j in range(chips):
        vn_copy(j).wait_send()


def solution(mesh):
    row_spec = P('data', 'seq', None)
    chips = mesh.shape['seq'] // CORES

    def local_block(act_in, ln1_scale, ln1_bias, w_in, b_in, ln2_scale, ln2_bias, w_spatial, b_spatial, causal_mask, w_out, b_out):
        batch, rows, model = act_in.shape
        ffn = w_in.shape[1]
        gate = w_out.shape[0]
        seq = w_spatial.shape[0]
        span = CORES * rows
        assert batch == chips and span * chips == seq
        n_out = 2 if model > 768 else 1
        assert chips == 4 and len(PLANS) == len(SENDS) == CORES * chips
        tiles = chips * (chips + 1) // 2
        hbm = pl.BlockSpec(memory_space=pl.ANY)
        vmem = pl.BlockSpec(memory_space=pltpu.VMEM)
        bf, f32 = jnp.bfloat16, jnp.float32
        dma = pltpu.SemaphoreType.DMA
        return pl.pallas_call(
            functools.partial(block_kernel, chips),
            out_shape=pltpu.VMEM(act_in.shape, bf),
            in_specs=[hbm, vmem, vmem, hbm, vmem, vmem, vmem, hbm, vmem, hbm, hbm, vmem],
            out_specs=hbm,
            scratch_shapes=[
                pltpu.VMEM((model, ffn), bf),
                pltpu.VMEM((gate, model), bf),
                pltpu.VMEM((chips, rows, model), bf),
                pltpu.VMEM((chips, rows, model), bf),
                pltpu.VMEM((rows, model), bf),
                pltpu.VMEM((rows, gate), bf),
                pltpu.VMEM((chips, rows, gate), bf),
                pltpu.VMEM((seq, gate), bf),
                pltpu.VMEM((chips, rows, seq), bf),
                pltpu.VMEM((tiles, rows, span), jnp.int32),
                pltpu.VMEM((rows, gate), bf),
                pltpu.VMEM((chips, rows, model), bf),
                pltpu.VMEM((chips, rows, 128), f32),
                pltpu.VMEM((1, model), f32),
                pltpu.VMEM((1, model), f32),
                pltpu.VMEM((1, ffn), f32),
                pltpu.VMEM((1, gate), f32),
                pltpu.VMEM((1, gate), f32),
                pltpu.VMEM((1, model), f32),
                dma((2,)), dma, dma((chips,)), dma((tiles,)), dma, dma,
                dma((chips,)), dma((chips,)), dma((chips,)), dma((chips,)),
                dma((chips, n_out)), dma((chips, n_out)), dma((n_out,)),
            ],
            compiler_params=pltpu.CompilerParams(collective_id=0, has_side_effects=True,
                                                 vmem_limit_bytes=62 * 1000 * 1000),
            name="gmlp_block",
        )(act_in, ln1_scale, ln1_bias, w_in, b_in, ln2_scale, ln2_bias, w_spatial, b_spatial, causal_mask, w_out, b_out)

    return jax.shard_map(local_block, mesh=mesh, in_specs=(row_spec,) + (P(),) * 11, out_specs=row_spec, check_vma=False)
```

```python
import functools

import jax
import jax.numpy as jnp
from jax import lax
from jax.experimental import pallas as pl
from jax.experimental.pallas import tpu as pltpu
from jax.sharding import PartitionSpec as P

LN_EPS = 1e-6
MESH = pl.DeviceIdType.MESH
GELU_A = 0.7978845608028654
GELU_B = 0.7978845608028654 * 0.044715
CORES = 2
HT = 256
NT = 512
OT = 256
PLANS = [
    [0, 1, 4, 2, 6, 3, 7, 5],
    [0, 1, 4, 2, 6, 3, 7, 5],
    [1, 2, 0, 3, 7, 6, 4, 5],
    [1, 2, 0, 3, 7, 6, 4, 5],
    [2, 1, 0, 4, 3, 7, 5, 6],
    [2, 1, 0, 4, 3, 7, 5, 6],
    [3, 0, 1, 5, 2, 4, 6, 7],
    [3, 0, 1, 5, 2, 4, 6, 7],
]
SENDS = [
    [(3, 0), (1, 1), (2, 2)],
    [(1, 0), (3, 1), (2, 2)],
    [(3, 0), (1, 0), (2, 2)],
    [(1, 0), (3, 1), (2, 2)],
    [(2, 0), (3, 0), (1, 1)],
    [(2, 0), (3, 1), (1, 2)],
    [(3, 0), (1, 2), (2, 2)],
    [(3, 0), (2, 2), (1, 2)],
]


def gelu(a):
    return (0.5 * a) * (1.0 + jnp.tanh(a * (GELU_A + GELU_B * (a * a))))


def norm_rows(src, dst, at, groups, width, scale, shift):
    tiles = [slice(t * 128, (t + 1) * 128) for t in range(width // 128)]
    rows = [pl.ds(pl.multiple_of(at[0] + 32 * r, 32), 32) for r in range(groups)]
    to = [pl.ds(pl.multiple_of(at[1] + 32 * r, 32), 32) for r in range(groups)]

    def total(parts):
        acc = parts[0]
        for p in parts[1:]:
            acc = acc + p
        return jnp.sum(acc, axis=-1, keepdims=True) * (1.0 / width)

    def load(r, t):
        return src[r, t].astype(jnp.float32)

    mean = [total([load(r, t) for t in tiles]) for r in rows]
    inv = []
    for r, m in zip(rows, mean):
        inv.append(lax.rsqrt(total([(load(r, t) - m) * (load(r, t) - m) for t in tiles]) + LN_EPS))
    for r, m, s, d in zip(rows, mean, inv, to):
        for t in tiles:
            dst[d, t] = ((load(r, t) - m) * s * scale[:, t] + shift[:, t]).astype(jnp.bfloat16)


def pick(me, values):
    out = values[-1]
    for d in range(len(values) - 1):
        out = jnp.where(me == d, values[d], out)
    return out


def packed(fields, bits):
    return sum(f << (bits * k) for k, f in enumerate(fields))


def partner_waits(plan, chips, core):
    seen, waits = set(), []
    for k, op in enumerate(plan):
        need = set(range(op - chips + core)) - seen if op >= chips else set()
        if k == len(plan) - 1:
            need = set(range(chips)) - seen
        seen |= need
        waits.append(sum(1 << j for j in need))
    assert waits[0] == 0
    return waits[1:]


def block_kernel(chips, x_hbm, ln1s_1d, ln1b_1d, w_in_hbm, b_in_1d, ln2s_1d, ln2b_1d, w_sp_hbm, b_sp_1d, mask_hbm,
                 w_out_hbm, b_out_1d, out_hbm,
                 w_in, w_out, xg, xs, u, v, g, vn, wm, mk, q, o, bs, ln1s, ln1b, b_in, ln2s, ln2b, b_out,
                 w_in_sem, w_out_sem, wm_sem, mk_sem, own_sem, xs_sem, x_send, x_recv, v_send, v_recv, o_send, o_recv, o_loc):
    rows, model = x_hbm.shape[1:]
    gate = w_out.shape[0]
    n_in = gate // NT
    span = CORES * rows
    data = lax.axis_index("data")
    me = lax.axis_index("seq")
    chip = me // CORES
    core = me % CORES

    def device(c):
        return (data, c * CORES + core)

    partner = (data, chip * CORES + (1 - core))

    barrier = pltpu.get_barrier_semaphore()
    for d in range(1, chips):
        pl.semaphore_signal(barrier, inc=1, device_id=device((chip + d) % chips), device_id_type=MESH)
    pl.semaphore_signal(barrier, inc=1, device_id=partner, device_id_type=MESH)

    own_copy = pltpu.make_async_copy(x_hbm.at[chip], xg.at[chip], own_sem)
    own_copy.start()
    w_in_copies = []
    for n in range(2):
        cols = pl.ds(gate * (1 - n), gate)
        w_in_copies.append(pltpu.make_async_copy(w_in_hbm.at[:, cols], w_in.at[:, cols], w_in_sem.at[n]))
    w_in_copies[0].start()
    for src, dst in ((ln1s_1d, ln1s), (ln1b_1d, ln1b), (b_in_1d, b_in), (ln2s_1d, ln2s), (ln2b_1d, ln2b),
                     (b_out_1d, b_out)):
        dst[...] = src[...].reshape(1, -1)

    pl.semaphore_wait(barrier, chips)

    def x_copy(d, src):
        to = (chip + d) % chips
        return pltpu.make_async_remote_copy(
            src_ref=src.at[to], dst_ref=xg.at[chip], send_sem=x_send.at[d], recv_sem=x_recv.at[d],
            device_id=device(to), device_id_type=MESH)

    sends = pick(me, [packed([d + (stage << 2) for d, stage in p], 4) for p in SENDS])

    def start_sends(stage, src):
        for slot in range(chips - 1):
            field = lax.shift_right_logical(sends, 4 * slot) % 16

            @pl.when(field // 4 == stage)
            def _(field=field):
                x_copy(field % 4, src).start()

    start_sends(0, x_hbm)
    w_in_copies[1].start()

    wm_copies, mk_copies = [], []
    t = 0
    for i in range(chips):
        r = pl.ds(pl.multiple_of((CORES * i + core) * rows, rows), rows)
        cp = pltpu.make_async_copy(w_sp_hbm.at[r, pl.ds(0, span * (i + 1))], wm.at[i, :, pl.ds(0, span * (i + 1))],
                                   wm_sem.at[i])
        cp.start()
        wm_copies.append(cp)
        for j in range(i + 1):
            cp = pltpu.make_async_copy(mask_hbm.at[r, pl.ds(span * j, span)], mk.at[t], mk_sem.at[t])
            cp.start()
            mk_copies.append(cp)
            t += 1
    w_out_copy = pltpu.make_async_copy(w_out_hbm, w_out, w_out_sem)
    w_out_copy.start()
    xs_copy = pltpu.make_async_copy(x_hbm, xs, xs_sem)
    xs_copy.start()

    def vn_copy(j):
        r = pl.ds(pl.multiple_of((CORES * j + core) * rows, rows), rows)
        return pltpu.make_async_remote_copy(
            src_ref=vn.at[r], dst_ref=vn.at[r], send_sem=v_send.at[j], recv_sem=v_recv.at[j],
            device_id=partner, device_id_type=MESH)

    def hidden(k, h, j):
        @pl.when(k == 0)
        def _():
            own_copy.wait()
            w_in_copies[0].wait()

        @pl.when(k > 0)
        def _():
            x_copy((chip - j + chips) % chips, xs).wait_recv()

        norm_rows(xg.at[j], u, (0, 0), rows // 32, model, ln1s, ln1b)

        def half(dst, base, first, last):
            def finish(n, a):
                a = a + b_in[:, base + n * HT:base + (n + 1) * HT]
                dst[:, n * HT:(n + 1) * HT] = gelu(a).astype(jnp.bfloat16)

            held = None
            for n in range(first, last):
                a = jnp.dot(u[...], w_in[:, base + n * HT:base + (n + 1) * HT], preferred_element_type=jnp.float32)
                if held is not None:
                    finish(n - 1, held)
                held = a
            finish(last - 1, held)

        half(v, gate, 0, gate // HT)

        own_rows = (CORES * j + core) * rows

        @pl.when(k == 0)
        def _():
            w_in_copies[1].wait()

        norm_rows(v, vn, (0, own_rows), rows // 32, gate, ln2s, ln2b)
        half(g.at[j], 0, 0, 5)
        vn_copy(j).start()

        @pl.when(h == 1)
        def _():
            xs_copy.wait()

        @pl.when(h > 0)
        def _():
            start_sends(h + 1, xs)

        half(g.at[j], 0, 5, gate // HT)

        @pl.when(h == 0)
        def _():
            start_sends(1, x_hbm)

    def mask_weights():
        for cp in wm_copies + mk_copies:
            cp.wait()
        t = 0
        for i in range(chips):
            for j in range(i + 1):
                cols = pl.ds(span * j, span)

                @pl.loop(0, rows // 32)
                def _(r, i=i, t=t, cols=cols):
                    rr = pl.ds(pl.multiple_of(r * 32, 32), 32)
                    w = wm[i, rr, cols].astype(jnp.float32)
                    wm[i, rr, cols] = jnp.where(mk[t, rr, :] > 0, w, 0.0).astype(jnp.bfloat16)

                t += 1
            row = b_sp_1d[pl.ds(pl.multiple_of((CORES * i + core) * rows, rows), rows)].reshape(1, rows)
            bs[i, :, :] = jnp.transpose(jnp.broadcast_to(row, (128, rows)))

    cuts = [(0, 768), (768, model)] if model > 768 else [(0, model)]

    def o_copy(i, n, recv):
        cols = pl.ds(cuts[n][0], cuts[n][1] - cuts[n][0])
        return pltpu.make_async_remote_copy(
            src_ref=o.at[i, :, cols], dst_ref=out_hbm.at[chip, :, cols], send_sem=o_send.at[i, n],
            recv_sem=o_recv.at[recv, n], device_id=device(i), device_id_type=MESH)

    def o_local(n):
        cols = pl.ds(cuts[n][0], cuts[n][1] - cuts[n][0])
        return pltpu.make_async_copy(o.at[chip, :, cols], out_hbm.at[chip, :, cols], o_loc.at[n])

    def mix(i, waits):
        for j in range(chips):
            @pl.when(lax.shift_right_logical(waits, j) % 2 == 1)
            def _(j=j):
                vn_copy(j).wait_recv()

        for s, c in [(s, c) for s in range(chips) for c in range(CORES)]:
            @pl.when((i == s) & (core == c))
            def _(s=s, depth=span * s + rows * (c + 1)):
                for n in range(n_in):
                    cols = slice(n * NT, (n + 1) * NT)
                    acc = jnp.dot(wm[s, :, :depth], vn[:depth, cols], preferred_element_type=jnp.float32)
                    sp = (acc + bs[s, :, 0:1]).astype(jnp.bfloat16).astype(jnp.float32)
                    q[:, cols] = (g[s, :, cols].astype(jnp.float32) * sp).astype(jnp.bfloat16)

        for n, (lo, hi) in enumerate(cuts):
            for c in range(lo, hi, OT):
                cols = slice(c, c + OT)
                y = jnp.dot(q[...], w_out[:, cols], preferred_element_type=jnp.float32) + b_out[:, cols]
                o[i, :, cols] = (xg[i, :, cols].astype(jnp.float32) + y).astype(jnp.bfloat16)

            @pl.when(i != chip)
            def _(n=n):
                o_copy(i, n, chip).start()

            @pl.when(i == chip)
            def _(n=n):
                o_local(n).start()

    plan = pick(me, [packed(p, 3) for p in PLANS])
    counts = pick(me, [packed([sum(o < chips for o in p[:k]) % 4 for k in range(len(p))], 2) for p in PLANS])
    plan_waits = pick(me, [packed(partner_waits(p, chips, d % CORES), chips) for d, p in enumerate(PLANS)])

    @pl.loop(0, 2 * chips)
    def _(k):
        op = lax.shift_right_logical(plan, 3 * k) % 8

        @pl.when(op < chips)
        def _():
            hidden(k, lax.shift_right_logical(counts, 2 * k) % 4, op)

        @pl.when(k == 0)
        def _():
            mask_weights()
            w_out_copy.wait()

        @pl.when(op >= chips)
        def _():
            mix(op - chips, lax.shift_right_logical(plan_waits, chips * (k - 1)) % (1 << chips))

    for d in range(1, chips):
        x_copy(d, xs).wait_send()
        src = (chip - d + chips) % chips
        for n in range(len(cuts)):
            o_copy(src, n, chip).wait_send()
            o_copy(src, n, src).wait_recv()
    for n in range(len(cuts)):
        o_local(n).wait()
    for j in range(chips):
        vn_copy(j).wait_send()


def solution(mesh):
    row_spec = P('data', 'seq', None)
    chips = mesh.shape['seq'] // CORES

    def local_block(act_in, ln1_scale, ln1_bias, w_in, b_in, ln2_scale, ln2_bias, w_spatial, b_spatial, causal_mask, w_out, b_out):
        batch, rows, model = act_in.shape
        ffn = w_in.shape[1]
        gate = w_out.shape[0]
        seq = w_spatial.shape[0]
        span = CORES * rows
        assert batch == chips and span * chips == seq
        n_out = 2 if model > 768 else 1
        assert chips == 4 and len(PLANS) == len(SENDS) == CORES * chips
        tiles = chips * (chips + 1) // 2
        hbm = pl.BlockSpec(memory_space=pl.ANY)
        vmem = pl.BlockSpec(memory_space=pltpu.VMEM)
        bf, f32 = jnp.bfloat16, jnp.float32
        dma = pltpu.SemaphoreType.DMA
        return pl.pallas_call(
            functools.partial(block_kernel, chips),
            out_shape=pltpu.VMEM(act_in.shape, bf),
            in_specs=[hbm, vmem, vmem, hbm, vmem, vmem, vmem, hbm, vmem, hbm, hbm, vmem],
            out_specs=hbm,
            scratch_shapes=[
                pltpu.VMEM((model, ffn), bf),
                pltpu.VMEM((gate, model), bf),
                pltpu.VMEM((chips, rows, model), bf),
                pltpu.VMEM((chips, rows, model), bf),
                pltpu.VMEM((rows, model), bf),
                pltpu.VMEM((rows, gate), bf),
                pltpu.VMEM((chips, rows, gate), bf),
                pltpu.VMEM((seq, gate), bf),
                pltpu.VMEM((chips, rows, seq), bf),
                pltpu.VMEM((tiles, rows, span), jnp.int32),
                pltpu.VMEM((rows, gate), bf),
                pltpu.VMEM((chips, rows, model), bf),
                pltpu.VMEM((chips, rows, 128), f32),
                pltpu.VMEM((1, model), f32),
                pltpu.VMEM((1, model), f32),
                pltpu.VMEM((1, ffn), f32),
                pltpu.VMEM((1, gate), f32),
                pltpu.VMEM((1, gate), f32),
                pltpu.VMEM((1, model), f32),
                dma((2,)), dma, dma((chips,)), dma((tiles,)), dma, dma,
                dma((chips,)), dma((chips,)), dma((chips,)), dma((chips,)),
                dma((chips, n_out)), dma((chips, n_out)), dma((n_out,)),
            ],
            compiler_params=pltpu.CompilerParams(collective_id=0, has_side_effects=True,
                                                 vmem_limit_bytes=62 * 1000 * 1000),
            name="gmlp_block",
        )(act_in, ln1_scale, ln1_bias, w_in, b_in, ln2_scale, ln2_bias, w_spatial, b_spatial, causal_mask, w_out, b_out)

    return jax.shard_map(local_block, mesh=mesh, in_specs=(row_spec,) + (P(),) * 11, out_specs=row_spec, check_vma=False)
```
